32 devices in a mesh: blk: 4 (over x, core), tp: 8 (over z, y).
Axes of the slice: x: 2, y: 2, z: 4, core: 2. Of those that a mesh axis runs over, the one named last changes fastest.
Arguments:
- residual_in: bfloat16 [2048, 5120], P('blk'), may hold values from -6 to 6
- norm_gain: bfloat16 [5120], replicated, may hold values from 0.099609375 to 1.8984375
- w_query: bfloat16 [5120, 4096], P(('blk', 'tp')), may hold values from -0.5 to 0.5
- w_key_value: bfloat16 [5120, 2048], P(('blk', 'tp')), may hold values from -0.5 to 0.5
- query_bias: bfloat16 [4096], replicated, may hold values from -3 to 3
- key_value_bias: bfloat16 [2048], replicated, may hold values from -3 to 3
- w_output: bfloat16 [4096, 5120], P(None, ('blk', 'tp')), may hold values from -0.09375 to 0.09375
- device_map: int32 [32], replicated, may hold values from 0 to 31, each once
- positions: int32 [2048], P('blk'), may hold values from 0 to 4094, as said below
- segments: int32 [2048], P('blk'), may hold values from 0 to 1, as said below
Outputs:
- output: bfloat16 [2048, 5120], P('blk', 'tp')
The draws below stay inside these ranges and needn't reach their ends.
Inputs may be any that keep to these rules, and one draw needn't show every extreme that they name: `segments`: ids never fall; both ids 0 and 1 occur; the shorter prompt holds a quarter of 512 up to 511 tokens. `positions`: a token's index within its prompt plus an offset shared by the whole prompt; the longer prompt's last token stands at 4094. `device_map`: each of 0 to 31 once.
All inputs are finite; a program needn't handle non-finite values.
Results may differ from the reference program's by a relative error of at most 0.012.
Values may be sent and summed in bfloat16 or wider, within the bound.
No kernel may reach another device: no remote copies, remote signals or barrier semaphores. Data moves between devices by JAX's collectives and lax.ppermute only.
A program may use at most 128 MiB of HBM per device.

```python
import jax
import jax.numpy as jnp
from jax import lax

D = 5120
HEADS = 32
KVH = 8
HD = 128
TOK_DEV = 512
LEN = 2048
QW = 4096
KVW = 2048
TRAINER_ROWS = 160
DEVICES = 32


def weight_pair(key):
    base_key = jax.random.fold_in(key, 11)
    query_key, pair_key = jax.random.split(base_key, 2)
    query_raw = jnp.clip(jax.random.normal(query_key, (D, KVH, HEADS // KVH, HD), jnp.float32), -6.0, 6.0)
    pairs_raw = jnp.clip(jax.random.normal(pair_key, (D, KVH, 2, HD), jnp.float32), -6.0, 6.0)
    fan_scale = D ** (-0.5)
    query_scaled = jnp.clip(query_raw.reshape(D, HEADS * HD) * fan_scale, -0.5, 0.5)
    pairs_scaled = jnp.clip(pairs_raw.reshape(D, 2 * KVH * HD) * fan_scale, -0.5, 0.5)
    return (query_scaled.astype(jnp.bfloat16), pairs_scaled.astype(jnp.bfloat16))


def prompt_layout(key):
    base_key = jax.random.fold_in(key, 23)
    short_key, order_key, offset_key = jax.random.split(base_key, 3)
    short_len = jax.random.randint(short_key, (), TOK_DEV // 4, TOK_DEV)
    first_short = jax.random.randint(order_key, (), 0, 2)
    boundary = jnp.where(first_short == 1, short_len, LEN - short_len)
    index_all = jnp.arange(LEN, dtype=jnp.int32)
    segment_ids = (index_all >= boundary).astype(jnp.int32)
    short_offset = jax.random.randint(offset_key, (), 0, 2048)
    long_offset = short_len + 2047
    offset_zero = jnp.where(first_short == 1, short_offset, long_offset)
    offset_one = jnp.where(first_short == 1, long_offset, short_offset)
    starts = jnp.where(segment_ids == 1, boundary, 0)
    shifted = jnp.where(segment_ids == 1, offset_one, offset_zero)
    return (segment_ids, (index_all - starts + shifted).astype(jnp.int32))


def draw_w_query(key, part):
    return weight_pair(key)[0]


def draw_w_key_value(key, part):
    return weight_pair(key)[1]


def draw_segments(key, part):
    return prompt_layout(key)[0]


def draw_positions(key, part):
    return prompt_layout(key)[1]


def level_of(own_key, extent, cuts, low, high):
    level, own = 1.0, jax.random.fold_in(own_key, 6)
    for position, shards_of in cuts:
        steps = jnp.exp(jax.random.uniform(jax.random.fold_in(own, position), (shards_of,), jnp.float32, low / len(cuts), high / len(cuts)))
        level = level * jnp.repeat(steps, extent[position] // shards_of).reshape([-1 if axis == position else 1 for axis in range(len(extent))])
    return level


def noise(key, extent, scale, limit, cuts=(), held_as=jnp.bfloat16):
    result = scale * jax.random.normal(key, extent, jnp.float32)
    if cuts:
        result = result * level_of(key, extent, cuts, -0.22, 0.18)
    return jnp.clip(result, -limit, limit).astype(held_as)


def setup_inputs(seed: int = 0) -> dict:
    splits = jax.random.split(jax.random.key(seed), 11)
    residual_in = noise(splits[0], (LEN, D), 1.0, 6.0, ((0, 4),))
    norm_gain = jnp.clip(1.0 + 0.18 * jax.random.normal(splits[1], (D,), jnp.float32), 0.099609375, 1.8984375).astype(jnp.bfloat16)
    w_query = draw_w_query(jax.random.fold_in(splits[10], 71), 0)
    w_key_value = draw_w_key_value(jax.random.fold_in(splits[10], 71), 0)
    query_bias = noise(splits[4], (QW,), 0.5, 3.0)
    key_value_bias = noise(splits[5], (KVW,), 0.5, 3.0)
    w_output = noise(splits[6], (QW, D), QW ** -0.5, 0.09375, ((1, 32),))
    device_map = jax.random.permutation(splits[7], DEVICES).astype(jnp.int32)
    positions = draw_positions(jax.random.fold_in(splits[10], 71), 0)
    segments = draw_segments(jax.random.fold_in(splits[10], 71), 0)
    return {"residual_in": residual_in, "norm_gain": norm_gain, "w_query": w_query, "w_key_value": w_key_value, "query_bias": query_bias, "key_value_bias": key_value_bias, "w_output": w_output, "device_map": device_map, "positions": positions, "segments": segments}


NORM_FLOOR = 0.0625
ROPE_BASE = 1000000.0
NEGATIVE_FILL = -1e+30

def rope_tables(positions, head_width):
    half_width = head_width // 2
    frequency = ROPE_BASE ** (-(jnp.arange(half_width, dtype=jnp.float32) * 2.0) / head_width)
    angles = positions.astype(jnp.float32)[:, None] * frequency[None, :]
    angles = jnp.concatenate([angles, angles], axis=1)
    return (jnp.cos(angles), jnp.sin(angles))

def rotate(values, cosine_table, sine_table):
    half_width = values.shape[-1] // 2
    turned = jnp.concatenate([-values[..., half_width:], values[..., :half_width]], axis=-1)
    return values * cosine_table[:, None, :] + turned * sine_table[:, None, :]

def reference(residual_in, norm_gain, w_query, w_key_value, query_bias, key_value_bias, w_output, device_map, positions, segments):
    floats = residual_in.astype(jnp.float32)
    square = jnp.maximum(lax.optimization_barrier(jnp.mean(floats * floats, axis=1, keepdims=True)), NORM_FLOOR)
    normed = (floats * lax.rsqrt(square) * norm_gain.astype(jnp.float32)).astype(jnp.bfloat16)
    ordered = jnp.take(normed.reshape(LEN, DEVICES, TRAINER_ROWS), device_map, axis=1).reshape(LEN, D)
    queries = jnp.dot(ordered, w_query, preferred_element_type=jnp.float32) + query_bias.astype(jnp.float32)
    key_value = jnp.dot(ordered, w_key_value, preferred_element_type=jnp.float32) + key_value_bias.astype(jnp.float32)
    cosine_table, sine_table = rope_tables(positions, HD)
    query_rot = rotate(queries.reshape(LEN, HEADS, HD), cosine_table, sine_table).astype(jnp.bfloat16)
    paired = key_value.reshape(LEN, KVH, 2, HD)
    key_rot = rotate(paired[:, :, 0, :], cosine_table, sine_table).astype(jnp.bfloat16)
    values = paired[:, :, 1, :].astype(jnp.bfloat16)
    per_group = HEADS // KVH
    query_rows = min(512, LEN)
    attend_scale = HD ** (-0.5)
    key_index = jnp.arange(LEN, dtype=jnp.int32)

    def one_block(block_number):
        block_start = (block_number * query_rows).astype(jnp.int32)
        query_block = lax.dynamic_slice_in_dim(query_rot, block_start, query_rows, 0)
        query_segment = lax.dynamic_slice_in_dim(segments, block_start, query_rows, 0)
        row_index = block_start + jnp.arange(query_rows, dtype=jnp.int32)
        visible = (key_index[None, :] <= row_index[:, None]) & (segments[None, :] == query_segment[:, None])

        def one_group(group_number):
            group_start = (group_number * per_group).astype(jnp.int32)
            query_group = lax.dynamic_slice_in_dim(query_block, group_start, per_group, 1).astype(jnp.float32)
            key_group = lax.dynamic_index_in_dim(key_rot, group_number, 1, keepdims=False).astype(jnp.float32)
            value_group = lax.dynamic_index_in_dim(values, group_number, 1, keepdims=False).astype(jnp.float32)
            scores = jnp.einsum('qhd,kd->hqk', query_group, key_group, precision=lax.Precision.HIGHEST) * attend_scale
            masked = jnp.where(visible[None], scores, NEGATIVE_FILL)
            row_peak = lax.optimization_barrier(jnp.max(masked, axis=2, keepdims=True))
            raw_weights = jnp.where(visible[None], jnp.exp(masked - row_peak), 0.0)
            weights = lax.optimization_barrier(raw_weights.astype(jnp.bfloat16)).astype(jnp.float32)
            context = jnp.einsum('hqk,kd->hqd', weights, value_group, precision=lax.Precision.HIGHEST)
            context = context / lax.optimization_barrier(jnp.sum(raw_weights, axis=2, keepdims=True))
            return context.astype(jnp.bfloat16)
        grouped = lax.map(one_group, jnp.arange(KVH, dtype=jnp.int32))
        return grouped.transpose(2, 0, 1, 3).reshape(query_rows, QW)
    blocks_out = lax.map(one_block, jnp.arange(LEN // query_rows, dtype=jnp.int32))
    context = blocks_out.reshape(LEN, QW)
    mixed = jnp.dot(context, w_output, preferred_element_type=jnp.float32)
    return (residual_in.astype(jnp.float32) + mixed).astype(jnp.bfloat16)
```

```python
import functools
import math

import jax
import jax.numpy as jnp
import numpy as np
from jax import lax
from jax.experimental import pallas as pl
from jax.experimental.pallas import tpu as pltpu
from jax.sharding import PartitionSpec as P

KVH = 8
HD = 128
NORM_FLOOR = 0.0625
ROPE_BASE = 1000000.0
NEGATIVE_FILL = -1e30
LOG2E = 1.4426950408889634
GROUP = 2


def xor_hop(block, axis, shift):
    count = lax.axis_size(axis)
    return lax.ppermute(block, axis, [(i, i ^ shift) for i in range(count)])


def blk_order(count):
    order = [0]
    bit = count >> 1
    while bit:
        order = order + [j ^ bit for j in order]
        bit >>= 1
    return order


def gather_blk(block):
    return finish_blk(*first_hop(block))


def first_hop(block):
    bit = lax.axis_size("blk") >> 1
    return (block, xor_hop(block, "blk", bit)) if bit else (block, None)


def finish_blk(block, other):
    gathered = jnp.stack([block, other])
    bit = lax.axis_size("blk") >> 2
    while bit:
        gathered = jnp.concatenate([gathered, xor_hop(gathered, "blk", bit)], axis=0)
        bit >>= 1
    return gathered


def rope_tables(positions):
    half = HD // 2
    frequency = ROPE_BASE ** (-(jnp.arange(half, dtype=jnp.float32) * 2.0) / HD)
    angles = positions.astype(jnp.float32)[:, None] * frequency[None, :]
    cosine, sine = jnp.cos(angles), jnp.sin(angles)
    return (
        jnp.concatenate([cosine, cosine], axis=1),
        jnp.concatenate([-sine, sine], axis=1),
    )


def order_body(map_ref, x_ref, gain_ref, out_ref, normed_ref, *, shard, window):
    width = x_ref.shape[1]
    floats = x_ref[...].astype(jnp.float32)
    square = jnp.maximum(jnp.mean(floats * floats, axis=1, keepdims=True), NORM_FLOOR)
    normed = (floats * lax.rsqrt(square) * gain_ref[...]).astype(jnp.bfloat16)
    normed_ref[:, :width] = normed.astype(jnp.float32)
    together = math.lcm(shard, 128) // shard
    for first in range(0, width // shard, together):
        parts = []
        for i in range(first, first + together):
            start = map_ref[i] * shard
            base = pl.multiple_of((start >> 7) << 7, 128)
            piece = normed_ref[:, pl.ds(base, window)]
            parts.append(pltpu.roll(piece, window - (start - base), 1)[:, :shard])
        out_ref[:, first * shard : (first + together) * shard] = jnp.concatenate(parts, axis=1).astype(jnp.bfloat16)


def ordered_norm(residual, gain, block_of, shard):
    tokens, width = residual.shape
    tile = min(128, tokens)
    window = -(-(128 - math.gcd(shard, 128) + shard) // 128) * 128
    return pl.pallas_call(
        functools.partial(order_body, shard=shard, window=window),
        grid_spec=pltpu.PrefetchScalarGridSpec(
            num_scalar_prefetch=1,
            grid=(tokens // tile,),
            in_specs=[
                pl.BlockSpec((tile, width), lambda i, m: (i, 0)),
                pl.BlockSpec((1, width), lambda i, m: (0, 0)),
            ],
            out_specs=pl.BlockSpec((tile, width), lambda i, m: (i, 0)),
            scratch_shapes=[pltpu.VMEM((tile, width + window), jnp.float32)],
        ),
        out_shape=jax.ShapeDtypeStruct((tokens, width), jnp.bfloat16),
        compiler_params=pltpu.CompilerParams(dimension_semantics=("arbitrary",)),
        name="order",
    )(block_of, residual, gain.astype(jnp.float32)[None, :])


def attend_body(q_ref, bias_ref, cos_ref, sin_ref, k_ref, v_ref, row_ref, col_ref, segq_ref, segk_ref, out_ref, mask_ref):
    @pl.when(pl.program_id(1) == 0)
    def _():
        visible = (col_ref[...] <= row_ref[...]) & (segk_ref[...] == segq_ref[...])
        mask_ref[...] = jnp.where(visible, 0.0, NEGATIVE_FILL)

    query = q_ref[...] + bias_ref[...]
    query = query * cos_ref[...] + pltpu.roll(query, HD // 2, 1) * sin_ref[...]
    scores = lax.dot_general(
        query.astype(jnp.bfloat16), k_ref[...], (((1,), (1,)), ((), ())),
        preferred_element_type=jnp.float32,
    )
    scores = scores + mask_ref[...]
    peak = jnp.max(scores, axis=1, keepdims=True)
    raw = jnp.exp2((scores - peak) * (HD ** (-0.5) * LOG2E))
    mass = jnp.sum(raw, axis=1, keepdims=True)
    context = jnp.dot(raw.astype(jnp.bfloat16), v_ref[...], preferred_element_type=jnp.float32)
    out_ref[...] = (context / mass).astype(jnp.bfloat16)


def attend(queries, bias, cosine, sine, keys, values, rows, cols, seg_q, seg_k):
    tokens, width = queries.shape
    length = keys.shape[0]
    tile = min(256, tokens)
    per_row = lambda w: pl.BlockSpec((tile, w), lambda i, h: (i, 0))
    whole = lambda a: pl.BlockSpec(a.shape, lambda i, h: (0, 0))
    return pl.pallas_call(
        attend_body,
        grid=(tokens // tile, width // HD),
        in_specs=[
            pl.BlockSpec((tile, HD), lambda i, h: (i, h)),
            pl.BlockSpec((1, HD), lambda i, h: (0, h)),
            per_row(HD), per_row(HD),
            whole(keys), whole(values),
            per_row(1), whole(cols), per_row(1), whole(seg_k),
        ],
        out_specs=pl.BlockSpec((tile, HD), lambda i, h: (i, h)),
        out_shape=jax.ShapeDtypeStruct((tokens, width), jnp.bfloat16),
        scratch_shapes=[pltpu.VMEM((tile, length), jnp.float32)],
        compiler_params=pltpu.CompilerParams(dimension_semantics=("arbitrary", "arbitrary")),
        name="attend",
    )(queries, bias, cosine, sine, keys, values, rows, cols, seg_q, seg_k)


def per_device(residual_in, norm_gain, w_query, w_key_value, query_bias, key_value_bias, w_output, device_map, positions, segments):
    n_tp, n_blk = lax.axis_size("tp"), lax.axis_size("blk")
    t, b = lax.axis_index("tp"), lax.axis_index("blk")
    tokens, width = residual_in.shape
    shard = w_query.shape[0]
    q_width = w_query.shape[1] // n_tp
    kv_width = 2 * HD
    kv_group = n_tp // KVH
    order = blk_order(n_blk)
    groups = [tuple(range(g, g + GROUP)) for g in range(0, n_tp, GROUP)]

    def kv_slice(dest):
        return lax.dynamic_slice_in_dim(w_key_value, (dest // kv_group) * kv_width, kv_width, 1)

    def q_slice(dest):
        return lax.dynamic_slice_in_dim(w_query, dest * q_width, q_width, 1)

    def moved(piece_of, group):
        pieces = [xor_hop(piece_of(t ^ s), "tp", s) if s else piece_of(t) for s in group]
        return jnp.stack(pieces)

    def whole_rows(halves):
        stacked = finish_blk(*halves)
        return stacked.reshape(-1, stacked.shape[-1])

    kv_pieces = [moved(kv_slice, g) for g in groups]
    q_pieces = [moved(q_slice, g) for g in groups]
    kv_halves = [first_hop(p) for p in kv_pieces]
    q_halves = [first_hop(p) for p in q_pieces]
    held = lax.optimization_barrier((residual_in, norm_gain, device_map, positions, segments, w_output, *kv_pieces))
    late_residual, norm_gain, device_map, positions, segments, w_output = held[:6]
    kv_weights = [whole_rows(h) for h in kv_halves]
    q_weights = [whole_rows(h) for h in q_halves]

    pairs = n_tp // 2
    pair_index, parity = t // 2, t % 2
    row_block = w_output.shape[0] // n_tp
    heads = q_width // HD
    chunks = 2 if heads % 2 == 0 else 1
    chunk_rows = row_block // chunks
    cols_here = w_output.shape[1]
    by_tp = w_output.reshape(pairs, 2, chunks, chunk_rows, cols_here)

    def out_rows(which):
        rows = lax.dynamic_index_in_dim(by_tp, which, 1, keepdims=False)
        rows = jnp.stack(
            [lax.dynamic_index_in_dim(rows, pair_index ^ i, 0, keepdims=False) for i in range(pairs)], axis=1
        )
        return rows.reshape(chunks * pairs * chunk_rows, cols_here).T

    out_pair = jnp.stack([out_rows(parity), xor_hop(out_rows(1 - parity), "tp", 1)])
    out_pair, late = lax.optimization_barrier((out_pair, q_halves[-1][1]))
    out_halves = first_hop(out_pair)

    j_of = np.array([j for g in groups for j in order for s in g], np.int32)
    s_of = np.array([s for g in groups for j in order for s in g], np.int32)
    block_of = jnp.take(device_map, (b ^ j_of) * n_tp + (t ^ s_of))
    ordered = ordered_norm(late_residual, norm_gain, block_of, shard)
    depth = GROUP * n_blk * shard

    def project(weights):
        total = None
        for i, w in enumerate(weights):
            part = jnp.dot(ordered[:, i * depth : (i + 1) * depth], w, preferred_element_type=jnp.float32)
            total = part if total is None else total + part
        return total

    cosine, sine = rope_tables(positions)
    key_value = project(kv_weights) + lax.dynamic_slice_in_dim(
        key_value_bias, (t // kv_group) * kv_width, kv_width
    ).astype(jnp.float32)
    keys = key_value[:, :HD]
    turned = jnp.concatenate([keys[:, HD // 2 :], keys[:, : HD // 2]], axis=1)
    keys = keys * cosine + turned * sine
    kv_block = jnp.stack([keys, key_value[:, HD:]]).astype(jnp.bfloat16)
    kv_all = gather_blk(kv_block)
    keys = kv_all[:, 0].reshape(n_blk * tokens, HD)
    values = kv_all[:, 1].reshape(n_blk * tokens, HD)
    blocks = b ^ np.array(order, np.int32)
    seg_k = gather_blk(segments).reshape(1, -1)
    cols = (blocks[:, None] * tokens + jnp.arange(tokens, dtype=jnp.int32)[None, :]).reshape(1, -1)
    rows = (b * tokens + jnp.arange(tokens, dtype=jnp.int32))[:, None]

    queries = project(q_weights)
    bias = lax.dynamic_slice_in_dim(query_bias, t * q_width, q_width).astype(jnp.float32)[None, :]

    partner_sum, own_sum = None, None
    gathered = []
    for c in range(chunks):
        span = slice(c * chunk_rows, (c + 1) * chunk_rows)
        context = attend(
            queries[:, span], bias[:, span], cosine, sine, keys, values, rows, cols, segments[:, None], seg_k
        )
        if c == chunks - 1:
            context, *out_halves = lax.optimization_barrier((context, *out_halves))
        gathered.append(
            jnp.concatenate([context] + [xor_hop(context, "tp", 2 * i) for i in range(1, pairs)], axis=1)
        )
    out_weights = finish_blk(*out_halves)
    for c in range(chunks):
        depth_here = pairs * chunk_rows
        weights_here = out_weights[:, :, :, c * depth_here : (c + 1) * depth_here]

        def product(which):
            return lax.dot_general(
                gathered[c], weights_here[:, which].reshape(n_blk * cols_here, depth_here),
                (((1,), (1,)), ((), ())), preferred_element_type=jnp.float32,
            )

        partner_sum = product(1) if partner_sum is None else partner_sum + product(1)
        own_sum = product(0) if own_sum is None else own_sum + product(0)
    received = xor_hop(partner_sum.astype(jnp.bfloat16), "tp", 1)
    summed = (own_sum + received.astype(jnp.float32)).reshape(tokens, n_blk, cols_here)

    spread = n_tp // n_blk
    position_of = np.argsort(np.array(order)).astype(np.int32)
    by_blk = summed.transpose(1, 0, 2).astype(jnp.bfloat16)
    place = t % n_blk
    arrived = []
    for r in range(n_blk):
        chosen = jnp.take(position_of, (r ^ place) ^ b)
        block = lax.dynamic_index_in_dim(by_blk, chosen, 0, keepdims=False)
        arrived.append(lax.ppermute(block, "tp", [(i, spread * (r ^ (i % n_blk)) + i // n_blk) for i in range(n_tp)]))
    arrived = jnp.stack(arrived)
    target = t // spread
    mixed = jnp.concatenate(
        [lax.dynamic_index_in_dim(arrived, target ^ o, 0, keepdims=False) for o in range(n_blk)], axis=1
    )
    width_out = width // n_tp
    residual_part = lax.dynamic_slice_in_dim(residual_in, t * width_out, width_out, 1)
    return (residual_part.astype(jnp.float32) + mixed.astype(jnp.float32)).astype(jnp.bfloat16)


def solution(mesh):
    in_specs = (
        P("blk", None),
        P(),
        P(("blk", "tp"), None),
        P(("blk", "tp"), None),
        P(),
        P(),
        P(None, ("blk", "tp")),
        P(),
        P("blk"),
        P("blk"),
    )
    return jax.shard_map(
        per_device, mesh=mesh, in_specs=in_specs, out_specs=P("blk", "tp"), check_vma=False
    )
```
